256 devices in a mesh: grp: 8 (over z), dev: 32 (over x, y, core).
Axes of the slice: x: 4, y: 4, z: 8, core: 2. Of those that a mesh axis runs over, the one named last changes fastest.
Arguments:
- blocks: bfloat16 [32768, 128, 128], P(('grp', 'dev')), may hold values from -0.29882812 to 0.29882812
- ids_one: int32 [2, 32768], P(None, ('grp', 'dev')), may hold values from 0 to 2047, as said below
- ids_two: int32 [2, 16384], P(None, ('grp', 'dev')), may hold values from 0 to 1023, as said below
- ids_three: int32 [2, 8192], P(None, ('grp', 'dev')), may hold values from 0 to 511
- match_one: int32 [2048, 128], replicated, may hold values from 0 to 127, as said below
- match_two: int32 [1024, 128], replicated, may hold values from 0 to 127, as said below
- match_three: int32 [512, 128], replicated, may hold values from 0 to 127, as said below
- target_one: int32 [32768], P(('grp', 'dev')), may hold values from 0 to 63
- target_two: int32 [16384], P(('grp', 'dev')), may hold values from 0 to 31
- target_three: int32 [8192], P(('grp', 'dev')), may hold values from 0 to 15
- vertex_weights: float32 [2048, 128], P(('grp', 'dev')), may hold values from 0.1 to 120, as said below
Outputs:
- coarse_graph: float32 [4096, 128, 128], P(('grp', 'dev'))
- rel_weight: float32 [256, 128], P(('grp', 'dev'))
The draws below stay inside these ranges and needn't reach their ends.
Inputs may be any that keep to these rules, and one draw needn't show every extreme that they name: `match_one`: rows 2b and 2b + 1 together name every number 0 to 127 exactly twice. `match_two`: rows 2b and 2b + 1 together name every number 0 to 127 exactly twice. `match_three`: rows 2b and 2b + 1 together name every number 0 to 127 exactly twice. `ids_one`: a fine block's row and column vertex blocks, halved by integer division, are the ids_two of the coarse slot it goes to. `ids_two`: a first-level block's row and column vertex blocks, halved by integer division, are the ids_three of the coarse slot it goes to. `vertex_weights`: positive.
All inputs are finite; a program needn't handle non-finite values.
Results may differ from the reference program's by a relative error of at most 0.0003.
Values may be sent and summed in bfloat16 or wider, within the bound.
A program may use at most 128 MiB of HBM per device.

```python
import math
import jax
import jax.numpy as jnp
from jax import lax

BLOCK = 128
SLOTS = 128
VWB = 8
NFINE = 32768
N_GRP = 8
N_DEV = 32
DEVICES = 256


def pairing(key, count):
    keys = jax.random.split(key, count // 2)
    perms = jax.vmap(lambda single: jax.random.permutation(single, 2 * BLOCK))(keys)
    return (perms // 2).reshape(count, BLOCK).astype(jnp.int32)


def route(count, per_dev, targets):
    slot = jnp.arange(count, dtype=jnp.int32)
    device = slot // per_dev
    local = slot % per_dev
    owner = device // N_DEV * N_DEV + local // (per_dev // N_DEV)
    return (owner * (per_dev // 2) + targets).astype(jnp.int32)


def layout(key):
    keys = jax.random.split(jax.random.fold_in(key, 7), 6)
    nfine = SLOTS * DEVICES
    vbzero = VWB * DEVICES
    ids_three = jax.random.randint(keys[0], (2, nfine // 4), 0, vbzero // 4, dtype=jnp.int32)
    target_two = jax.random.randint(keys[1], (nfine // 2,), 0, SLOTS // 4, dtype=jnp.int32)
    dest_two = route(nfine // 2, SLOTS // 2, target_two)
    ids_two = 2 * ids_three[:, dest_two] + jax.random.randint(keys[2], (2, nfine // 2), 0, 2, dtype=jnp.int32)
    target_one = jax.random.randint(keys[3], (nfine,), 0, SLOTS // 2, dtype=jnp.int32)
    dest_one = route(nfine, SLOTS, target_one)
    ids_one = 2 * ids_two[:, dest_one] + jax.random.randint(keys[4], (2, nfine), 0, 2, dtype=jnp.int32)
    target_three = jax.random.randint(keys[5], (nfine // 4,), 0, SLOTS // 8, dtype=jnp.int32)
    return (ids_one.astype(jnp.int32), ids_two.astype(jnp.int32), ids_three.astype(jnp.int32), target_one, target_two, target_three)


def draw_ids_one(key, part):
    return layout(key)[0]


def draw_ids_two(key, part):
    return layout(key)[1]


def draw_ids_three(key, part):
    return layout(key)[2]


def draw_target_one(key, part):
    return layout(key)[3]


def draw_target_two(key, part):
    return layout(key)[4]


def draw_target_three(key, part):
    return layout(key)[5]


def draw_match_one(key, part):
    return pairing(jax.random.fold_in(key, 11), VWB * DEVICES)


def draw_match_two(key, part):
    return pairing(jax.random.fold_in(key, 12), VWB * DEVICES // 2)


def draw_match_three(key, part):
    return pairing(jax.random.fold_in(key, 13), VWB * DEVICES // 4)


def draw_vertex_weights(key, part):
    first, second = jax.random.split(jax.random.fold_in(key, 21))
    count = VWB * DEVICES
    scale = jnp.exp(jax.random.uniform(first, (count, 1), jnp.float32, 0.0, math.log(16.0)))
    values = jax.random.uniform(second, (count, BLOCK), jnp.float32, 0.5, 1.5)
    return (scale * values).astype(jnp.float32)


def block_levels(own_key, extent, cuts, least, high):
    level = 1.0
    for position, shards_of in cuts:
        draws = jax.random.uniform(jax.random.fold_in(jax.random.fold_in(own_key, 6), position), (shards_of,), jnp.float32, least / len(cuts), high / len(cuts))
        level = level * jnp.repeat(jnp.exp(draws), extent[position] // shards_of).reshape((-1,) + (1,) * (len(extent) - 1 - position))
    return level


def scatter_about(own_key, dims, spread, reach, shards=(), kind=jnp.bfloat16):
    array = jax.random.normal(own_key, dims, jnp.float32) * spread
    if len(shards) > 0:
        array = block_levels(own_key, dims, shards, -0.22, 0.18) * array
    return jnp.clip(array, min=-reach, max=reach).astype(kind)


def setup_inputs(seed: int = 0) -> dict:
    key_list = jax.random.split(jax.random.key(seed), 12)
    return {
        "blocks": scatter_about(key_list[0], (NFINE, BLOCK, BLOCK), 0.05, 0.29882812, ((0, 256),)),
        "ids_one": draw_ids_one(jax.random.fold_in(key_list[11], 71), 0),
        "ids_two": draw_ids_two(jax.random.fold_in(key_list[11], 71), 0),
        "ids_three": draw_ids_three(jax.random.fold_in(key_list[11], 71), 0),
        "match_one": draw_match_one(jax.random.fold_in(key_list[11], 71), 0),
        "match_two": draw_match_two(jax.random.fold_in(key_list[11], 71), 0),
        "match_three": draw_match_three(jax.random.fold_in(key_list[11], 71), 0),
        "target_one": draw_target_one(jax.random.fold_in(key_list[11], 71), 0),
        "target_two": draw_target_two(jax.random.fold_in(key_list[11], 71), 0),
        "target_three": draw_target_three(jax.random.fold_in(key_list[11], 71), 0),
        "vertex_weights": draw_vertex_weights(jax.random.fold_in(key_list[11], 71), 0),
    }


def project_blocks(blocks, pair_ids, table):
    row_map = table[pair_ids[0]]
    col_map = table[pair_ids[1]]

    def single(matrix, rows, cols):
        halfway = jax.ops.segment_sum(matrix.astype(jnp.float32), rows, num_segments=BLOCK)
        return jax.ops.segment_sum(halfway.T, cols, num_segments=BLOCK).T

    return jax.vmap(single)(blocks, row_map, col_map)


def coarsen(blocks, pair_ids, table, targets, per_dev, fold_groups):
    count = blocks.shape[0]
    slot = jnp.arange(count, dtype=jnp.int32)
    device = slot // per_dev
    local = slot % per_dev
    group = device // N_DEV
    member = device % N_DEV
    if fold_groups:
        owner = (local // (per_dev // N_GRP)) * N_DEV + member
    else:
        owner = group * N_DEV + local // (per_dev // N_DEV)
    dest = (owner * (per_dev // 2) + targets).astype(jnp.int32)
    width = math.gcd(count, 512)
    turns = count // width
    inputs = (blocks.reshape(turns, width, BLOCK, BLOCK),
              pair_ids.reshape(2, turns, width).transpose(1, 0, 2),
              dest.reshape(turns, width))

    def accumulate(total, piece):
        part = project_blocks(piece[0], piece[1], table)
        return total.at[piece[2]].add(part), None

    start = jnp.zeros((count // 2, BLOCK, BLOCK), jnp.float32)
    coarse, _ = lax.scan(accumulate, start, inputs)
    return coarse


def pair_weights(weights, table):
    count = weights.shape[0]
    index = (jnp.arange(count, dtype=jnp.int32)[:, None] // 2) * BLOCK + table.astype(jnp.int32)
    summed = jax.ops.segment_sum(weights.reshape(-1), index.reshape(-1), num_segments=count // 2 * BLOCK)
    return summed.reshape(count // 2, BLOCK)


def reference(blocks, ids_one, ids_two, ids_three, match_one, match_two, match_three, target_one, target_two, target_three, vertex_weights):
    coarse_one = coarsen(blocks, ids_one, match_one, target_one, SLOTS, False)
    coarse_two = coarsen(coarse_one, ids_two, match_two, target_two, SLOTS // 2, False)
    coarse_graph = coarsen(coarse_two, ids_three, match_three, target_three, SLOTS // 4, True)
    weights_three = pair_weights(pair_weights(pair_weights(vertex_weights, match_one), match_two), match_three)
    total = jnp.sum(vertex_weights)
    rel_weight = weights_three * (weights_three.shape[0] * BLOCK) / total
    return coarse_graph, rel_weight
```

```python
import functools

import jax
import jax.numpy as jnp
from jax import lax
from jax.experimental import pallas as pl
from jax.experimental.pallas import tpu as pltpu
from jax.sharding import PartitionSpec as P

MESH = pl.DeviceIdType.MESH
BLOCK = 128
PITCH = 136
CHUNKS = 2
ROWS = BLOCK // CHUNKS
SPAN = ROWS + 8
TOP = 32767.0
TINY = 1e-30
ROUNDS = (
    ((0, 0),),
    ((0, 1), (1, 1), (0, 3), (3, 3)),
    ((1, 0), (1, 3), (3, 0), (3, 1)),
    ((0, 2), (2, 1), (2, 3)),
    ((2, 0), (1, 2), (3, 2)),
    ((2, 2),),
)
ORDER = tuple(
    (dx, dy, dc) for turn in ROUNDS for dc in (0, 1) for dx, dy in turn if (dx, dy, dc) != (0, 0, 0)
)
RING = (1, 7, 2, 6, 3, 5, 4)


def dest_of(v, dx, dy, dc):
    x, y, c = v // 8, lax.rem(v // 2, 4), lax.rem(v, 2)
    ddx = jnp.where(c == 1, dy, dx)
    ddy = jnp.where(c == 1, dx, dy)
    return lax.rem(x + ddx, 4) * 8 + lax.rem(y + ddy, 4) * 2 + lax.rem(c + dc, 2)


def source_of(v, turn):
    code = jnp.int32(0)
    for place, (dx, dy, dc) in enumerate(ORDER):
        code = jnp.where(turn == place + 1, dx * 8 + dy * 2 + dc, code)
    dx, dy, dc = code // 8, lax.rem(code // 2, 4), lax.rem(code, 2)
    x, y, c = v // 8, lax.rem(v // 2, 4), lax.rem(v, 2)
    other = lax.rem(c + dc, 2)
    ddx = jnp.where(other == 1, dy, dx)
    ddy = jnp.where(other == 1, dx, dy)
    return lax.rem(x + 4 - ddx, 4) * 8 + lax.rem(y + 4 - ddy, 4) * 2 + other


def split(value):
    high = value.astype(jnp.bfloat16)
    return high, (value - high.astype(jnp.float32)).astype(jnp.bfloat16)


def one_hot(lanes, count):
    width = lanes.shape[1]
    rows = lax.broadcasted_iota(jnp.int32, (count, width), 0).astype(jnp.float32)
    return jnp.where(rows == lanes, 1.0, 0.0).astype(jnp.bfloat16)


def send(src, dst, send_sem, recv_sem, device):
    pltpu.make_async_remote_copy(
        src_ref=src, dst_ref=dst, send_sem=send_sem, recv_sem=recv_sem, device_id=device, device_id_type=MESH
    ).start()


def wait(ref, sem):
    pltpu.make_async_copy(ref, ref, sem).wait()


def kernel(
    blocks, ids, one, two, three, target_one, target_two, target_three, weights,
    graph, relative,
    fine, maps_out, maps_in, tags_out, tags_in, zags_out, zags_in, projected, coarse_one, out_two, in_two,
    size_two, sizein_two, spread, coarse_two, out_three, in_three, size_three, sizein_three, weighted,
    fine_send, fine_recv, maps_sem, tags_sem, zags_sem, two_sem, sizetwo_sem, three_sem, sizethree_sem,
):
    g, v = lax.axis_index("grp"), lax.axis_index("dev")
    barrier = pltpu.get_barrier_semaphore()
    for step in ORDER:
        pl.semaphore_signal(barrier, inc=1, device_id=(g, dest_of(v, *step)), device_id_type=MESH)
    for step in RING:
        pl.semaphore_signal(barrier, inc=1, device_id=(lax.rem(g + step, 8), v), device_id_type=MESH)
    mine = pltpu.make_async_copy(blocks.at[pl.ds(v * 4, 4)], fine.at[pl.ds(v * 4, 4)], fine_recv.at[v])
    mine.start()

    def composed(numbers):
        first = jnp.concatenate([one[pl.ds(n, 1), :] for n in numbers], axis=0)
        second = jnp.concatenate([two[pl.ds(n // 2, 1), :] for n in numbers], axis=0)
        third = jnp.concatenate([three[pl.ds(n // 4, 1), :] for n in numbers], axis=0)
        second = jnp.take_along_axis(second, first, axis=1)
        return jnp.take_along_axis(third, second, axis=1).astype(jnp.float32)

    def make_maps(w, carry):
        numbers = [ids[a, w * 4 + j] for a in range(2) for j in range(4)]
        maps_out[w] = composed(numbers).astype(jnp.bfloat16)
        return carry

    lax.fori_loop(0, 32, make_maps, 0)
    maps_in[v] = maps_out[v]

    lane = lax.broadcasted_iota(jnp.int32, (32, BLOCK), 1)
    row = lax.broadcasted_iota(jnp.int32, (32, BLOCK), 0)
    local = weights[...]
    partial = jnp.sum(jnp.sum(local, axis=0, keepdims=True), axis=1, keepdims=True)

    def spread_tags(table, per, count, place):
        index = lax.rem(count * 0 + row * per + lax.rem(lane, per), BLOCK)
        picked = jnp.take_along_axis(jnp.broadcast_to(table, (32, BLOCK)), index, axis=1)
        return jnp.where(lane // per == place, picked, 0).astype(jnp.float32)

    tags_one = spread_tags(target_one[...], 4, 32, v)
    tags_two = spread_tags(target_two[...], 2, 32, v)
    tags_two = tags_two + jnp.where(lane == v + 64, partial, 0.0)
    for w in range(32):
        tags_out[w, 0:1, :] = tags_one[w : w + 1]
        tags_out[w, 1:2, :] = tags_two[w : w + 1]
    tags_in[v] = tags_out[v]

    pl.semaphore_wait(barrier, len(ORDER) + len(RING))
    for step in ORDER:
        w = dest_of(v, *step)
        send(maps_out.at[w], maps_in.at[v], maps_sem.at[0], maps_sem.at[1], (g, w))
        send(tags_out.at[w], tags_in.at[v], tags_sem.at[0], tags_sem.at[1], (g, w))
    for place, step in enumerate(ORDER):
        w = dest_of(v, *step)
        send(
            blocks.at[pl.ds(w * 4, 4)], fine.at[pl.ds(v * 4, 4)], fine_send.at[place], fine_recv.at[v], (g, w)
        )

    base = (g * 32 + v) * 8
    own = composed([base + e for e in range(8)])
    part = lax.broadcasted_iota(jnp.int32, (8, BLOCK), 0)
    total_here = jnp.zeros((8, BLOCK), jnp.float32)
    up = lax.broadcasted_iota(jnp.int32, (BLOCK, BLOCK), 0).astype(jnp.float32)
    for e in range(8):
        hot = jnp.where(up == own[e : e + 1], 1.0, 0.0)
        total_here = total_here + lax.dot_general(
            jnp.where(part == e, local, 0.0), hot, (((1,), (1,)), ((), ())),
            precision=lax.Precision.HIGHEST, preferred_element_type=jnp.float32,
        )
    weighted[...] = jnp.sum(total_here, axis=0, keepdims=True)

    wait(maps_in.at[pl.ds(0, 31)], maps_sem.at[1])
    wait(tags_in.at[pl.ds(0, 31)], tags_sem.at[1])

    def project(turn, carry):
        s = source_of(v, turn)
        wait(fine.at[pl.ds(s * 4, 4)], fine_recv.at[s])
        maps = maps_in[s].astype(jnp.float32)
        for j in range(4):
            left = one_hot(maps[j : j + 1], BLOCK)
            right = one_hot(maps[4 + j : 5 + j], BLOCK)
            halfway = jnp.dot(left, fine[s * 4 + j], preferred_element_type=jnp.float32)
            both = jnp.concatenate(split(halfway), axis=0)
            full = lax.dot_general(
                both, right, (((1,), (1,)), ((), ())), preferred_element_type=jnp.float32
            )
            start = pl.multiple_of((s * 4 + j) * PITCH, 8)
            projected[pl.ds(start, BLOCK), :] = full[:BLOCK] + full[BLOCK:]
        return carry

    lax.fori_loop(0, 32, project, 0)

    tags = jnp.sum(tags_in[...], axis=0)
    hot_one = one_hot(tags[0:1], 64)
    hot_one = jnp.concatenate([hot_one, hot_one], axis=1)
    hot_two = one_hot(tags[1:2], 32)[:, :64]
    hot_two = jnp.concatenate([hot_two, hot_two], axis=1)
    beyond = lax.broadcasted_iota(jnp.int32, (1, BLOCK), 1)
    group_total = jnp.sum(jnp.where(beyond >= 64, tags[1:2], 0.0), axis=1, keepdims=True)

    lane8 = lax.broadcasted_iota(jnp.int32, (8, BLOCK), 1)
    row8 = lax.broadcasted_iota(jnp.int32, (8, BLOCK), 0)
    picked = jnp.take_along_axis(
        jnp.broadcast_to(target_three[...], (8, BLOCK)), row8 * 4 + lax.rem(lane8, 4), axis=1
    )
    tags_three = jnp.where(lane8 // 4 == g, picked, 0).astype(jnp.float32)
    totals = jnp.where(beyond == g, group_total, 0.0)
    for h in range(8):
        zags_out[h, 0:1, :] = tags_three[h : h + 1]
        zags_out[h, 1:2, :] = totals
    zags_in[g] = zags_out[g]
    for step in RING:
        h = lax.rem(g + step, 8)
        send(zags_out.at[h], zags_in.at[g], zags_sem.at[0], zags_sem.at[1], (h, v))

    def quantize(source, count, chunk, out, size, per):
        def one_block(s, carry):
            value = source[pl.ds(pl.multiple_of(s * PITCH + chunk * ROWS, 8), ROWS), :]
            top = jnp.max(jnp.abs(value), axis=0, keepdims=True)
            top = jnp.maximum(top, TINY)
            scaled = jnp.round(value * (TOP / top))
            out[chunk, s] = scaled.astype(jnp.int32).astype(jnp.int16)
            size[chunk, s] = top
            return carry

        lax.fori_loop(0, count, one_block, 0, unroll=4)

    def restore(source, size, count, chunk):
        def one_block(s, carry):
            value = source[chunk, s].astype(jnp.int32).astype(jnp.float32)
            spread[pl.ds(pl.multiple_of(s * SPAN, 8), ROWS), :] = value * (size[chunk, s] * (1.0 / TOP))
            return carry

        lax.fori_loop(0, count, one_block, 0, unroll=4)

    def add_up(source, pitch, count, first, hot, store):
        def one_row(m, carry):
            value = source[pl.ds(first + m, count, stride=pitch), :]
            both = jnp.concatenate(split(value), axis=0)
            store(m, jnp.dot(hot, both, preferred_element_type=jnp.float32))
            return carry

        lax.fori_loop(0, ROWS, one_row, 0, unroll=8)

    for chunk in range(CHUNKS):

        def keep_one(m, value, chunk=chunk):
            coarse_one[pl.ds(chunk * ROWS + m, 64, stride=PITCH), :] = value

        add_up(projected, PITCH, BLOCK, chunk * ROWS, hot_one, keep_one)
        quantize(coarse_one, 64, chunk, out_two, size_two, 2)
        here = pl.ds(v * 2, 2)
        in_two[chunk, here] = out_two[chunk, here]
        sizein_two[chunk, here] = size_two[chunk, here]
        for step in ORDER:
            w = dest_of(v, *step)
            there = pl.ds(w * 2, 2)
            send(
                size_two.at[chunk, there], sizein_two.at[chunk, here],
                sizetwo_sem.at[0, chunk], sizetwo_sem.at[1, chunk], (g, w),
            )
            send(
                out_two.at[chunk, there], in_two.at[chunk, here],
                two_sem.at[0, chunk], two_sem.at[1, chunk], (g, w),
            )

    wait(zags_in.at[pl.ds(0, 7)], zags_sem.at[1])
    zags = jnp.sum(zags_in[...], axis=0)
    hot_three = one_hot(zags[0:1], 16)[:, :32]
    hot_three = jnp.concatenate([hot_three, hot_three], axis=1)
    relative[...] = weighted[...] * 32768.0 / jnp.sum(zags[1:2], axis=1, keepdims=True)

    for chunk in range(CHUNKS):
        wait(sizein_two.at[chunk, pl.ds(0, 62)], sizetwo_sem.at[1, chunk])
        wait(in_two.at[chunk, pl.ds(0, 62)], two_sem.at[1, chunk])
        restore(in_two, sizein_two, 64, chunk)

        def keep_two(m, value, chunk=chunk):
            coarse_two[pl.ds(chunk * ROWS + m, 32, stride=PITCH), :] = value

        add_up(spread, SPAN, 64, 0, hot_two, keep_two)
        quantize(coarse_two, 32, chunk, out_three, size_three, 4)
        here = pl.ds(g * 4, 4)
        in_three[chunk, here] = out_three[chunk, here]
        sizein_three[chunk, here] = size_three[chunk, here]
        for step in RING:
            h = lax.rem(g + step, 8)
            there = pl.ds(h * 4, 4)
            send(
                size_three.at[chunk, there], sizein_three.at[chunk, here],
                sizethree_sem.at[0, chunk], sizethree_sem.at[1, chunk], (h, v),
            )
            send(
                out_three.at[chunk, there], in_three.at[chunk, here],
                three_sem.at[0, chunk], three_sem.at[1, chunk], (h, v),
            )

    for chunk in range(CHUNKS):
        wait(sizein_three.at[chunk, pl.ds(0, 28)], sizethree_sem.at[1, chunk])
        wait(in_three.at[chunk, pl.ds(0, 28)], three_sem.at[1, chunk])
        restore(in_three, sizein_three, 32, chunk)

        def keep_three(m, value, chunk=chunk):
            graph[pl.ds(chunk * ROWS + m, 16, stride=BLOCK), :] = value

        add_up(spread, SPAN, 32, 0, hot_three, keep_three)

    for place, step in enumerate(ORDER):
        w = dest_of(v, *step)
        wait(blocks.at[pl.ds(w * 4, 4)], fine_send.at[place])
    wait(maps_in.at[pl.ds(0, 31)], maps_sem.at[0])
    wait(tags_in.at[pl.ds(0, 31)], tags_sem.at[0])
    wait(zags_in.at[pl.ds(0, 7)], zags_sem.at[0])
    for chunk in range(CHUNKS):
        wait(size_two.at[chunk, pl.ds(0, 62)], sizetwo_sem.at[0, chunk])
        wait(out_two.at[chunk, pl.ds(0, 62)], two_sem.at[0, chunk])
        wait(size_three.at[chunk, pl.ds(0, 28)], sizethree_sem.at[0, chunk])
        wait(out_three.at[chunk, pl.ds(0, 28)], three_sem.at[0, chunk])


def pad_lanes(values):
    return jnp.pad(values, (0, BLOCK - values.shape[0])).reshape(1, BLOCK)


def per_device(
    blocks, ids_one, ids_two, ids_three, match_one, match_two, match_three,
    target_one, target_two, target_three, vertex_weights,
):
    del ids_two, ids_three
    vmem = pl.BlockSpec(memory_space=pltpu.VMEM)
    f32, i16, bf16 = jnp.float32, jnp.int16, jnp.bfloat16
    graph, relative = pl.pallas_call(
        kernel,
        out_shape=(
            jax.ShapeDtypeStruct((16 * BLOCK, BLOCK), f32),
            jax.ShapeDtypeStruct((1, BLOCK), f32),
        ),
        in_specs=[pl.BlockSpec(memory_space=pl.ANY), pl.BlockSpec(memory_space=pltpu.SMEM)] + [vmem] * 7,
        out_specs=(vmem, vmem),
        scratch_shapes=[
            pltpu.VMEM((128, BLOCK, BLOCK), bf16),
            pltpu.VMEM((32, 8, BLOCK), bf16),
            pltpu.VMEM((32, 8, BLOCK), bf16),
            pltpu.VMEM((32, 2, BLOCK), f32),
            pltpu.VMEM((32, 2, BLOCK), f32),
            pltpu.VMEM((8, 2, BLOCK), f32),
            pltpu.VMEM((8, 2, BLOCK), f32),
            pltpu.VMEM((128 * PITCH, BLOCK), f32),
            pltpu.VMEM((64 * PITCH, BLOCK), f32),
            pltpu.VMEM((CHUNKS, 64, ROWS, BLOCK), i16),
            pltpu.VMEM((CHUNKS, 64, ROWS, BLOCK), i16),
            pltpu.VMEM((CHUNKS, 64, 1, BLOCK), f32),
            pltpu.VMEM((CHUNKS, 64, 1, BLOCK), f32),
            pltpu.VMEM((64 * SPAN, BLOCK), f32),
            pltpu.VMEM((32 * PITCH, BLOCK), f32),
            pltpu.VMEM((CHUNKS, 32, ROWS, BLOCK), i16),
            pltpu.VMEM((CHUNKS, 32, ROWS, BLOCK), i16),
            pltpu.VMEM((CHUNKS, 32, 1, BLOCK), f32),
            pltpu.VMEM((CHUNKS, 32, 1, BLOCK), f32),
            pltpu.VMEM((1, BLOCK), f32),
            pltpu.SemaphoreType.DMA((31,)),
            pltpu.SemaphoreType.DMA((32,)),
            pltpu.SemaphoreType.DMA((2,)),
            pltpu.SemaphoreType.DMA((2,)),
            pltpu.SemaphoreType.DMA((2,)),
            pltpu.SemaphoreType.DMA((2, CHUNKS)),
            pltpu.SemaphoreType.DMA((2, CHUNKS)),
            pltpu.SemaphoreType.DMA((2, CHUNKS)),
            pltpu.SemaphoreType.DMA((2, CHUNKS)),
        ],
        compiler_params=pltpu.CompilerParams(
            collective_id=0, has_side_effects=True, vmem_limit_bytes=56 * 2**20
        ),
        name="coarsen",
    )(
        blocks, ids_one, match_one, match_two, match_three,
        target_one.reshape(1, BLOCK), pad_lanes(target_two), pad_lanes(target_three), vertex_weights,
    )
    return graph.reshape(16, BLOCK, BLOCK), relative


def solution(mesh):
    both = ("grp", "dev")
    in_specs = (
        P(both, None, None), P(None, both), P(None, both), P(None, both), P(), P(), P(),
        P(both), P(both), P(both), P(both, None),
    )
    return jax.shard_map(
        per_device, mesh=mesh, in_specs=in_specs, out_specs=(P(both, None, None), P(both, None)), check_vma=False
    )
```

```python
import functools

import jax
import jax.numpy as jnp
from jax import lax
from jax.experimental import pallas as pl
from jax.experimental.pallas import tpu as pltpu
from jax.sharding import PartitionSpec as P

MESH = pl.DeviceIdType.MESH
BLOCK = 128
PITCH = 136
CHUNKS = 8
AHEAD = 3
FIRST = 5
ROWS = BLOCK // CHUNKS
SPAN = ROWS + 8
TOP = 32767.0
TINY = 1e-30
ROUNDS = (
    ((0, 0),),
    ((0, 1), (1, 1), (0, 3), (3, 3)),
    ((1, 0), (1, 3), (3, 0), (3, 1)),
    ((0, 2), (2, 1), (2, 3)),
    ((2, 0), (1, 2), (3, 2)),
    ((2, 2),),
)
ORDER = tuple(
    (dx, dy, dc) for turn in ROUNDS for dc in (0, 1) for dx, dy in turn if (dx, dy, dc) != (0, 0, 0)
)
RING = (1, 7, 2, 6, 3, 5, 4)


def dest_of(v, dx, dy, dc):
    x, y, c = v // 8, lax.rem(v // 2, 4), lax.rem(v, 2)
    ddx = jnp.where(c == 1, dy, dx)
    ddy = jnp.where(c == 1, dx, dy)
    return lax.rem(x + ddx, 4) * 8 + lax.rem(y + ddy, 4) * 2 + lax.rem(c + dc, 2)


def source_of(v, turn):
    code = jnp.int32(0)
    for place, (dx, dy, dc) in enumerate(ORDER):
        code = jnp.where(turn == place + 1, dx * 8 + dy * 2 + dc, code)
    dx, dy, dc = code // 8, lax.rem(code // 2, 4), lax.rem(code, 2)
    x, y, c = v // 8, lax.rem(v // 2, 4), lax.rem(v, 2)
    other = lax.rem(c + dc, 2)
    ddx = jnp.where(other == 1, dy, dx)
    ddy = jnp.where(other == 1, dx, dy)
    return lax.rem(x + 4 - ddx, 4) * 8 + lax.rem(y + 4 - ddy, 4) * 2 + other


def split(value):
    high = value.astype(jnp.bfloat16)
    return high, (value - high.astype(jnp.float32)).astype(jnp.bfloat16)


def one_hot(lanes, count):
    width = lanes.shape[1]
    rows = lax.broadcasted_iota(jnp.int32, (count, width), 0).astype(jnp.float32)
    return jnp.where(rows == lanes, 1.0, 0.0).astype(jnp.bfloat16)


def send(src, dst, send_sem, recv_sem, device):
    pltpu.make_async_remote_copy(
        src_ref=src, dst_ref=dst, send_sem=send_sem, recv_sem=recv_sem, device_id=device, device_id_type=MESH
    ).start()


def wait(ref, sem):
    pltpu.make_async_copy(ref, ref, sem).wait()


def kernel(
    blocks, ids, one_hbm, two_hbm, three_hbm, target_one, target_two, target_three, weights,
    graph, relative,
    fine, maps_out, maps_in, tags_out, tags_in, zags_out, zags_in, projected, coarse_one, out_two, in_two,
    size_two, sizein_two, spread, coarse_two, out_three, in_three, size_three, sizein_three, weighted,
    one, two, three, tables_sem, fine_send, fine_recv, maps_sem, tags_sem, zags_sem, two_sem, sizetwo_sem, three_sem, sizethree_sem,
):
    g, v = lax.axis_index("grp"), lax.axis_index("dev")
    barrier = pltpu.get_barrier_semaphore()
    for step in ORDER:
        pl.semaphore_signal(barrier, inc=1, device_id=(g, dest_of(v, *step)), device_id_type=MESH)
    for step in RING:
        pl.semaphore_signal(barrier, inc=1, device_id=(lax.rem(g + step, 8), v), device_id_type=MESH)
    tables = [
        pltpu.make_async_copy(source, table, tables_sem.at[place])
        for place, (source, table) in enumerate(((one_hbm, one), (two_hbm, two), (three_hbm, three)))
    ]
    for table in tables:
        table.start()
    mine = pltpu.make_async_copy(blocks.at[pl.ds(v * 4, 4)], fine.at[pl.ds(v * 4, 4)], fine_recv.at[v])
    mine.start()

    def send_fine(place):
        w = dest_of(v, *ORDER[place])
        send(
            blocks.at[pl.ds(w * 4, 4)], fine.at[pl.ds(v * 4, 4)], fine_send.at[place], fine_recv.at[v], (g, w)
        )

    pl.semaphore_wait(barrier, len(ORDER) + len(RING))
    for place in range(FIRST):
        send_fine(place)
    for table in tables:
        table.wait()

    def composed(numbers):
        first = jnp.concatenate([one[pl.ds(n, 1), :] for n in numbers], axis=0)
        second = jnp.concatenate([two[pl.ds(n // 2, 1), :] for n in numbers], axis=0)
        third = jnp.concatenate([three[pl.ds(n // 4, 1), :] for n in numbers], axis=0)
        second = jnp.take_along_axis(second, first, axis=1)
        return jnp.take_along_axis(third, second, axis=1).astype(jnp.float32)

    def make_maps(w, carry):
        numbers = [ids[a, w * 4 + j] for a in range(2) for j in range(4)]
        maps_out[w] = composed(numbers).astype(jnp.bfloat16)
        return carry

    lax.fori_loop(0, 32, make_maps, 0)
    maps_in[v] = maps_out[v]

    lane = lax.broadcasted_iota(jnp.int32, (32, BLOCK), 1)
    row = lax.broadcasted_iota(jnp.int32, (32, BLOCK), 0)
    local = weights[...]
    partial = jnp.sum(jnp.sum(local, axis=0, keepdims=True), axis=1, keepdims=True)

    def spread_tags(table, per, rows, lanes, place):
        table = jnp.concatenate([table] * (BLOCK // table.shape[1]), axis=1)
        table = jnp.broadcast_to(table, lanes.shape)
        picked = jnp.take_along_axis(table, rows * per + lax.rem(lanes, per), axis=1)
        return jnp.where(lanes // per == place, picked, 0).astype(jnp.float32)

    tags_one = spread_tags(target_one[...], 4, row, lane, v)
    tags_two = spread_tags(target_two[...], 2, row, lane, v)
    tags_two = tags_two + jnp.where(lane == v + 64, partial, 0.0)
    for w in range(32):
        tags_out[w, 0:1, :] = tags_one[w : w + 1]
        tags_out[w, 1:2, :] = tags_two[w : w + 1]
    tags_in[v] = tags_out[v]

    for step in ORDER:
        w = dest_of(v, *step)
        send(maps_out.at[w], maps_in.at[v], maps_sem.at[0], maps_sem.at[1], (g, w))
        send(tags_out.at[w], tags_in.at[v], tags_sem.at[0], tags_sem.at[1], (g, w))
    for place in range(FIRST, len(ORDER)):
        send_fine(place)

    base = (g * 32 + v) * 8
    own = composed([base + e for e in range(8)])
    part = lax.broadcasted_iota(jnp.int32, (8, BLOCK), 0)
    total_here = jnp.zeros((8, BLOCK), jnp.float32)
    up = lax.broadcasted_iota(jnp.int32, (BLOCK, BLOCK), 0).astype(jnp.float32)
    for e in range(8):
        hot = jnp.where(up == own[e : e + 1], 1.0, 0.0)
        total_here = total_here + lax.dot_general(
            jnp.where(part == e, local, 0.0), hot, (((1,), (1,)), ((), ())),
            precision=lax.Precision.HIGHEST, preferred_element_type=jnp.float32,
        )
    weighted[...] = jnp.sum(total_here, axis=0, keepdims=True)

    wait(maps_in.at[pl.ds(0, 31)], maps_sem.at[1])
    wait(tags_in.at[pl.ds(0, 31)], tags_sem.at[1])

    tags = jnp.sum(tags_in[...], axis=0)
    hot_one = one_hot(tags[0:1], 64)
    hot_one = jnp.concatenate([hot_one, hot_one], axis=1)
    hot_two = one_hot(tags[1:2], 32)[:, :64]
    hot_two = jnp.concatenate([hot_two, hot_two], axis=1)
    beyond = lax.broadcasted_iota(jnp.int32, (1, BLOCK), 1)
    group_total = jnp.sum(jnp.where(beyond >= 64, tags[1:2], 0.0), axis=1, keepdims=True)

    lane8 = lax.broadcasted_iota(jnp.int32, (8, BLOCK), 1)
    row8 = lax.broadcasted_iota(jnp.int32, (8, BLOCK), 0)
    tags_three = spread_tags(target_three[...], 4, row8, lane8, g)
    totals = jnp.where(beyond == g, group_total, 0.0)
    for h in range(8):
        zags_out[h, 0:1, :] = tags_three[h : h + 1]
        zags_out[h, 1:2, :] = totals
    zags_in[g] = zags_out[g]
    for step in RING:
        h = lax.rem(g + step, 8)
        send(zags_out.at[h], zags_in.at[g], zags_sem.at[0], zags_sem.at[1], (h, v))

    def project(turn, carry):
        s = source_of(v, turn)
        wait(fine.at[pl.ds(s * 4, 4)], fine_recv.at[s])
        maps = maps_in[s].astype(jnp.float32)
        for j in range(4):
            left = one_hot(maps[j : j + 1], BLOCK)
            right = one_hot(maps[4 + j : 5 + j], BLOCK)
            halfway = jnp.dot(left, fine[s * 4 + j], preferred_element_type=jnp.float32)
            both = jnp.concatenate(split(halfway), axis=0)
            full = lax.dot_general(
                both, right, (((1,), (1,)), ((), ())), preferred_element_type=jnp.float32
            )
            start = pl.multiple_of((s * 4 + j) * PITCH, 8)
            projected[pl.ds(start, BLOCK), :] = full[:BLOCK] + full[BLOCK:]
        return carry

    lax.fori_loop(0, 32, project, 0)

    def quantize(source, count, per, chunk, out, size):
        def one_group(w, carry):
            values = [
                source[pl.ds(pl.multiple_of((w * per + k) * PITCH + chunk * ROWS, 8), ROWS), :] for k in range(per)
            ]
            top = functools.reduce(jnp.maximum, [jnp.max(jnp.abs(a), axis=0, keepdims=True) for a in values])
            top = jnp.maximum(top, TINY)
            factor = TOP / top
            for k, a in enumerate(values):
                out[chunk, w * per + k] = jnp.round(a * factor).astype(jnp.int32).astype(jnp.int16)
            size[chunk, w] = top * (1.0 / TOP)
            return carry

        lax.fori_loop(0, count, one_group, 0, unroll=2)

    def restore(source, size, count, per, chunk):
        def one_group(w, carry):
            for k in range(per):
                s = w * per + k
                value = source[chunk, s].astype(jnp.int32).astype(jnp.float32)
                spread[pl.ds(pl.multiple_of(s * SPAN, 8), ROWS), :] = value * size[chunk, w]
            return carry

        lax.fori_loop(0, count, one_group, 0, unroll=2)

    def add_up(source, pitch, count, first, hot, store):
        def one_row(m, carry):
            value = source[pl.ds(first + m, count, stride=pitch), :]
            both = jnp.concatenate(split(value), axis=0)
            store(m, jnp.dot(hot, both, preferred_element_type=jnp.float32))
            return carry

        lax.fori_loop(0, ROWS, one_row, 0, unroll=8)

    def make_two(chunk):
        def keep(m, value):
            coarse_one[pl.ds(chunk * ROWS + m, 64, stride=PITCH), :] = value

        add_up(projected, PITCH, BLOCK, chunk * ROWS, hot_one, keep)
        quantize(coarse_one, 32, 2, chunk, out_two, size_two)
        here = pl.ds(v * 2, 2)
        in_two[chunk, here] = out_two[chunk, here]
        sizein_two[chunk, v] = size_two[chunk, v]

    def sends_two(chunk, step):
        w = dest_of(v, *step)
        send(
            size_two.at[chunk, w], sizein_two.at[chunk, v],
            sizetwo_sem.at[0, chunk], sizetwo_sem.at[1, chunk], (g, w),
        )
        send(
            out_two.at[chunk, pl.ds(w * 2, 2)], in_two.at[chunk, pl.ds(v * 2, 2)],
            two_sem.at[0, chunk], two_sem.at[1, chunk], (g, w),
        )

    def make_three(chunk):
        def keep(m, value):
            coarse_two[pl.ds(chunk * ROWS + m, 32, stride=PITCH), :] = value

        wait(sizein_two.at[chunk, pl.ds(0, 31)], sizetwo_sem.at[1, chunk])
        wait(in_two.at[chunk, pl.ds(0, 62)], two_sem.at[1, chunk])
        restore(in_two, sizein_two, 32, 2, chunk)
        add_up(spread, SPAN, 64, 0, hot_two, keep)
        quantize(coarse_two, 8, 4, chunk, out_three, size_three)
        here = pl.ds(g * 4, 4)
        in_three[chunk, here] = out_three[chunk, here]
        sizein_three[chunk, g] = size_three[chunk, g]

    def sends_three(chunk, step):
        h = lax.rem(g + step, 8)
        send(
            size_three.at[chunk, h], sizein_three.at[chunk, g],
            sizethree_sem.at[0, chunk], sizethree_sem.at[1, chunk], (h, v),
        )
        send(
            out_three.at[chunk, pl.ds(h * 4, 4)], in_three.at[chunk, pl.ds(g * 4, 4)],
            three_sem.at[0, chunk], three_sem.at[1, chunk], (h, v),
        )

    for chunk in range(AHEAD):
        make_two(chunk)
        for step in ORDER:
            sends_two(chunk, step)
    wait(zags_in.at[pl.ds(0, 7)], zags_sem.at[1])
    zags = jnp.sum(zags_in[...], axis=0)
    hot_three = one_hot(zags[0:1], 16)[:, :32]
    hot_three = jnp.concatenate([hot_three, hot_three], axis=1)
    relative[...] = weighted[...] * 32768.0 / jnp.sum(zags[1:2], axis=1, keepdims=True)
    for chunk in range(CHUNKS):
        ahead = chunk + AHEAD
        if ahead < CHUNKS:
            make_two(ahead)
        make_three(chunk)
        for place, step in enumerate(ORDER if ahead < CHUNKS else RING * 4):
            if place % 4 == 0 and place // 4 < len(RING):
                sends_three(chunk, RING[place // 4])
            if ahead < CHUNKS:
                sends_two(ahead, step)

    for chunk in range(CHUNKS):
        wait(sizein_three.at[chunk, pl.ds(0, 7)], sizethree_sem.at[1, chunk])
        wait(in_three.at[chunk, pl.ds(0, 28)], three_sem.at[1, chunk])
        restore(in_three, sizein_three, 8, 4, chunk)

        def keep_three(m, value, chunk=chunk):
            graph[pl.ds(chunk * ROWS + m, 16, stride=BLOCK), :] = value

        add_up(spread, SPAN, 32, 0, hot_three, keep_three)

    for place, step in enumerate(ORDER):
        w = dest_of(v, *step)
        wait(blocks.at[pl.ds(w * 4, 4)], fine_send.at[place])
    wait(maps_in.at[pl.ds(0, 31)], maps_sem.at[0])
    wait(tags_in.at[pl.ds(0, 31)], tags_sem.at[0])
    wait(zags_in.at[pl.ds(0, 7)], zags_sem.at[0])
    for chunk in range(CHUNKS):
        wait(size_two.at[chunk, pl.ds(0, 31)], sizetwo_sem.at[0, chunk])
        wait(out_two.at[chunk, pl.ds(0, 62)], two_sem.at[0, chunk])
        wait(size_three.at[chunk, pl.ds(0, 7)], sizethree_sem.at[0, chunk])
        wait(out_three.at[chunk, pl.ds(0, 28)], three_sem.at[0, chunk])


def per_device(
    blocks, ids_one, ids_two, ids_three, match_one, match_two, match_three,
    target_one, target_two, target_three, vertex_weights,
):
    del ids_two, ids_three
    vmem = pl.BlockSpec(memory_space=pltpu.VMEM)
    hbm = pl.BlockSpec(memory_space=pl.ANY)
    f32, i16, bf16 = jnp.float32, jnp.int16, jnp.bfloat16
    graph, relative = pl.pallas_call(
        kernel,
        out_shape=(
            jax.ShapeDtypeStruct((16 * BLOCK, BLOCK), f32),
            jax.ShapeDtypeStruct((1, BLOCK), f32),
        ),
        in_specs=[hbm, pl.BlockSpec(memory_space=pltpu.SMEM), hbm, hbm, hbm] + [vmem] * 4,
        out_specs=(vmem, vmem),
        scratch_shapes=[
            pltpu.VMEM((128, BLOCK, BLOCK), bf16),
            pltpu.VMEM((32, 8, BLOCK), bf16),
            pltpu.VMEM((32, 8, BLOCK), bf16),
            pltpu.VMEM((32, 2, BLOCK), f32),
            pltpu.VMEM((32, 2, BLOCK), f32),
            pltpu.VMEM((8, 2, BLOCK), f32),
            pltpu.VMEM((8, 2, BLOCK), f32),
            pltpu.VMEM((128 * PITCH, BLOCK), f32),
            pltpu.VMEM((64 * PITCH, BLOCK), f32),
            pltpu.VMEM((CHUNKS, 64, ROWS, BLOCK), i16),
            pltpu.VMEM((CHUNKS, 64, ROWS, BLOCK), i16),
            pltpu.VMEM((CHUNKS, 32, 1, BLOCK), f32),
            pltpu.VMEM((CHUNKS, 32, 1, BLOCK), f32),
            pltpu.VMEM((64 * SPAN, BLOCK), f32),
            pltpu.VMEM((32 * PITCH, BLOCK), f32),
            pltpu.VMEM((CHUNKS, 32, ROWS, BLOCK), i16),
            pltpu.VMEM((CHUNKS, 32, ROWS, BLOCK), i16),
            pltpu.VMEM((CHUNKS, 8, 1, BLOCK), f32),
            pltpu.VMEM((CHUNKS, 8, 1, BLOCK), f32),
            pltpu.VMEM((1, BLOCK), f32),
            pltpu.VMEM(match_one.shape, jnp.int32),
            pltpu.VMEM(match_two.shape, jnp.int32),
            pltpu.VMEM(match_three.shape, jnp.int32),
            pltpu.SemaphoreType.DMA((3,)),
            pltpu.SemaphoreType.DMA((31,)),
            pltpu.SemaphoreType.DMA((32,)),
            pltpu.SemaphoreType.DMA((2,)),
            pltpu.SemaphoreType.DMA((2,)),
            pltpu.SemaphoreType.DMA((2,)),
            pltpu.SemaphoreType.DMA((2, CHUNKS)),
            pltpu.SemaphoreType.DMA((2, CHUNKS)),
            pltpu.SemaphoreType.DMA((2, CHUNKS)),
            pltpu.SemaphoreType.DMA((2, CHUNKS)),
        ],
        compiler_params=pltpu.CompilerParams(
            collective_id=0, has_side_effects=True, vmem_limit_bytes=56 * 2**20
        ),
        name="coarsen",
    )(
        blocks, ids_one, match_one, match_two, match_three,
        target_one.reshape(1, -1), target_two.reshape(1, -1), target_three.reshape(1, -1), vertex_weights,
    )
    return graph.reshape(16, BLOCK, BLOCK), relative


def solution(mesh):
    both = ("grp", "dev")
    in_specs = (
        P(both, None, None), P(None, both), P(None, both), P(None, both), P(), P(), P(),
        P(both), P(both), P(both), P(both, None),
    )
    return jax.shard_map(
        per_device, mesh=mesh, in_specs=in_specs, out_specs=(P(both, None, None), P(both, None)), check_vma=False
    )
```

```python
import functools

import jax
import jax.numpy as jnp
from jax import lax
from jax.experimental import pallas as pl
from jax.experimental.pallas import tpu as pltpu
from jax.sharding import PartitionSpec as P

MESH = pl.DeviceIdType.MESH
BLOCK = 128
CHUNKS = 8
EARLY = 4
AHEAD = 3
HALF = BLOCK // 2
ROWS = BLOCK // CHUNKS
SPAN = ROWS + 8
TOP = 32767.0
TINY = 1e-30
ROUNDS = (
    ((0, 0),),
    ((0, 1), (1, 1), (0, 3), (3, 3)),
    ((1, 0), (1, 3), (3, 0), (3, 1)),
    ((0, 2), (2, 1), (2, 3)),
    ((2, 0), (1, 2), (3, 2)),
    ((2, 2),),
)
ORDER = tuple(
    (dx, dy, dc) for turn in ROUNDS for dc in (0, 1) for dx, dy in turn if (dx, dy, dc) != (0, 0, 0)
)
RING = (1, 7, 2, 6, 3, 5, 4)


def dest_of(v, dx, dy, dc):
    x, y, c = v // 8, lax.rem(v // 2, 4), lax.rem(v, 2)
    ddx = jnp.where(c == 1, dy, dx)
    ddy = jnp.where(c == 1, dx, dy)
    return lax.rem(x + ddx, 4) * 8 + lax.rem(y + ddy, 4) * 2 + lax.rem(c + dc, 2)


def dest_at(v, turn):
    code = jnp.int32(0)
    for place, (dx, dy, dc) in enumerate(ORDER):
        code = jnp.where(turn == place + 1, dx * 8 + dy * 2 + dc, code)
    return dest_of(v, code // 8, lax.rem(code // 2, 4), lax.rem(code, 2))


def split(value):
    high = value.astype(jnp.bfloat16)
    return high, (value - high.astype(jnp.float32)).astype(jnp.bfloat16)


def one_hot(lanes, count):
    width = lanes.shape[1]
    rows = lax.broadcasted_iota(jnp.int32, (count, width), 0).astype(jnp.float32)
    return jnp.where(rows == lanes, 1.0, 0.0).astype(jnp.bfloat16)


def send(src, dst, send_sem, recv_sem, device):
    pltpu.make_async_remote_copy(
        src_ref=src, dst_ref=dst, send_sem=send_sem, recv_sem=recv_sem, device_id=device, device_id_type=MESH
    ).start()


def wait(ref, sem):
    pltpu.make_async_copy(ref, ref, sem).wait()


def kernel(
    blocks, ids, one_hbm, two_hbm, three_hbm, target_one, target_two, target_three, weights,
    graph, relative,
    fine, out_one, in_one, size_one, sizein_one, tags_out, tags_in, zags_out, zags_in, coarse_one, out_two, in_two,
    size_two, sizein_two, spread, coarse_two, out_three, in_three, size_three, sizein_three, weighted,
    one, two, three, maps, projected, tables_sem, fine_sem, one_sem, sizeone_sem, tags_sem, zags_sem,
    two_sem, sizetwo_sem, three_sem, sizethree_sem,
):
    g, v = lax.axis_index("grp"), lax.axis_index("dev")
    barrier = pltpu.get_barrier_semaphore()
    for step in ORDER:
        pl.semaphore_signal(barrier, inc=1, device_id=(g, dest_of(v, *step)), device_id_type=MESH)
    for step in RING:
        pl.semaphore_signal(barrier, inc=1, device_id=(lax.rem(g + step, 8), v), device_id_type=MESH)
    tables = [
        pltpu.make_async_copy(source, table, tables_sem.at[place])
        for place, (source, table) in enumerate(((one_hbm, one), (two_hbm, two), (three_hbm, three)))
    ]
    for table in tables:
        table.start()
    for place, step in enumerate(((0, 0, 0),) + ORDER):
        some = pl.ds(dest_of(v, *step) * 4, 4)
        pltpu.make_async_copy(blocks.at[some], fine.at[some], fine_sem.at[place]).start()

    def composed(numbers):
        first = jnp.concatenate([one[pl.ds(n, 1), :] for n in numbers], axis=0)
        second = jnp.concatenate([two[pl.ds(n // 2, 1), :] for n in numbers], axis=0)
        third = jnp.concatenate([three[pl.ds(n // 4, 1), :] for n in numbers], axis=0)
        second = jnp.take_along_axis(second, first, axis=1)
        return jnp.take_along_axis(third, second, axis=1).astype(jnp.float32)

    lane = lax.broadcasted_iota(jnp.int32, (32, BLOCK), 1)
    row = lax.broadcasted_iota(jnp.int32, (32, BLOCK), 0)
    local = weights[...]
    partial = jnp.sum(jnp.sum(local, axis=0, keepdims=True), axis=1, keepdims=True)

    def spread_tags(table, per, rows, lanes, place):
        table = jnp.concatenate([table] * (BLOCK // table.shape[1]), axis=1)
        table = jnp.broadcast_to(table, lanes.shape)
        picked = jnp.take_along_axis(table, rows * per + lax.rem(lanes, per), axis=1)
        return jnp.where(lanes // per == place, picked, 0).astype(jnp.float32)

    tags_one = spread_tags(target_one[...], 4, row, lane, v)
    tags_two = spread_tags(target_two[...], 2, row, lane, v)
    tags_two = tags_two + jnp.where(lane == v + 64, partial, 0.0)
    for w in range(32):
        tags_out[w, 0:1, :] = tags_one[w : w + 1]
        tags_out[w, 1:2, :] = tags_two[w : w + 1]
    tags_in[v] = tags_out[v]

    for table in tables:
        table.wait()

    def find_maps(turn):
        w = dest_at(v, turn)
        maps[...] = composed([ids[a, w * 4 + j] for a in range(2) for j in range(4)])

    def project(turn):
        w = dest_at(v, turn)
        wait(fine.at[pl.ds(w * 4, 4)], fine_sem.at[turn])
        here = maps[...]
        for j in range(4):
            left = one_hot(here[j : j + 1], BLOCK)
            right = one_hot(here[4 + j : 5 + j], BLOCK)
            halfway = jnp.dot(left, fine[w * 4 + j], preferred_element_type=jnp.float32)
            both = jnp.concatenate(split(halfway), axis=0)
            full = lax.dot_general(both, right, (((1,), (1,)), ((), ())), preferred_element_type=jnp.float32)
            projected[j * BLOCK : (j + 1) * BLOCK, :] = full[:BLOCK] + full[BLOCK:]

    def round_one(turn):
        w = dest_at(v, turn)
        for pair in range(2):
            for half in range(2):
                starts = [(pair * 2 + k) * BLOCK + half * HALF for k in range(2)]
                values = [projected[start : start + HALF, :] for start in starts]
                top = jnp.maximum(*[jnp.max(jnp.abs(a), axis=0, keepdims=True) for a in values])
                top = jnp.maximum(top, TINY)
                factor = TOP / top
                for k, a in enumerate(values):
                    out_one[half, w * 4 + pair * 2 + k] = jnp.round(a * factor).astype(jnp.int32).astype(jnp.int16)
                size_one[half, w, pair : pair + 1, :] = top * (1.0 / TOP)

    def send_one(half, turn):
        w = dest_at(v, turn)
        send(
            size_one.at[half, w], sizein_one.at[half, v], sizeone_sem.at[0, half], sizeone_sem.at[1, half], (g, w)
        )
        send(
            out_one.at[half, pl.ds(w * 4, 4)], in_one.at[half, pl.ds(v * 4, 4)],
            one_sem.at[0, half], one_sem.at[1, half], (g, w),
        )

    find_maps(0)
    project(0)
    find_maps(1)
    pl.semaphore_wait(barrier, len(ORDER) + len(RING))
    for step in ORDER:
        w = dest_of(v, *step)
        send(tags_out.at[w], tags_in.at[v], tags_sem.at[0], tags_sem.at[1], (g, w))

    def step_on(turn, carry):
        round_one(turn - 1)
        project(turn)
        find_maps(jnp.minimum(turn + 1, 31))

        @pl.when(turn >= 3)
        def _():
            send_one(0, turn - 2)

        return carry

    lax.fori_loop(1, 32, step_on, 0)
    send_one(0, 30)
    round_one(31)
    send_one(0, 31)
    lax.fori_loop(1, 32, lambda turn, carry: (send_one(1, turn), carry)[1], 0)
    for half in range(2):
        in_one[half, pl.ds(v * 4, 4)] = out_one[half, pl.ds(v * 4, 4)]
        sizein_one[half, v] = size_one[half, v]

    base = (g * 32 + v) * 8
    own = composed([base + e for e in range(8)])
    part = lax.broadcasted_iota(jnp.int32, (8, BLOCK), 0)
    total_here = jnp.zeros((8, BLOCK), jnp.float32)
    up = lax.broadcasted_iota(jnp.int32, (BLOCK, BLOCK), 0).astype(jnp.float32)
    for e in range(8):
        hot = jnp.where(up == own[e : e + 1], 1.0, 0.0)
        total_here = total_here + lax.dot_general(
            jnp.where(part == e, local, 0.0), hot, (((1,), (1,)), ((), ())),
            precision=lax.Precision.HIGHEST, preferred_element_type=jnp.float32,
        )
    weighted[...] = jnp.sum(total_here, axis=0, keepdims=True)

    wait(tags_in.at[pl.ds(0, 31)], tags_sem.at[1])
    tags = jnp.sum(tags_in[...], axis=0)
    hot_one = one_hot(tags[0:1], 64)
    hot_one = jnp.concatenate([hot_one, hot_one], axis=1)
    hot_two = one_hot(tags[1:2], 32)[:, :64]
    hot_two = jnp.concatenate([hot_two, hot_two], axis=1)
    beyond = lax.broadcasted_iota(jnp.int32, (1, BLOCK), 1)
    group_total = jnp.sum(jnp.where(beyond >= 64, tags[1:2], 0.0), axis=1, keepdims=True)

    lane8 = lax.broadcasted_iota(jnp.int32, (8, BLOCK), 1)
    row8 = lax.broadcasted_iota(jnp.int32, (8, BLOCK), 0)
    tags_three = spread_tags(target_three[...], 4, row8, lane8, g)
    totals = jnp.where(beyond == g, group_total, 0.0)
    for h in range(8):
        zags_out[h, 0:1, :] = tags_three[h : h + 1]
        zags_out[h, 1:2, :] = totals
    zags_in[g] = zags_out[g]
    for step in RING:
        h = lax.rem(g + step, 8)
        send(zags_out.at[h], zags_in.at[g], zags_sem.at[0], zags_sem.at[1], (h, v))

    def quantize(source, count, per, chunk, out, size):
        def one_group(w, carry):
            values = [
                source[pl.ds(pl.multiple_of((w * per + k) * SPAN, 8), ROWS), :] for k in range(per)
            ]
            top = functools.reduce(jnp.maximum, [jnp.max(jnp.abs(a), axis=0, keepdims=True) for a in values])
            top = jnp.maximum(top, TINY)
            factor = TOP / top
            for k, a in enumerate(values):
                out[chunk, w * per + k] = jnp.round(a * factor).astype(jnp.int32).astype(jnp.int16)
            size[chunk, w] = top * (1.0 / TOP)
            return carry

        lax.fori_loop(0, count, one_group, 0, unroll=2)

    def restore(source, size, count, per, chunk):
        def one_group(w, carry):
            for k in range(per):
                s = w * per + k
                value = source[chunk, s].astype(jnp.int32).astype(jnp.float32)
                spread[pl.ds(pl.multiple_of(s * SPAN, 8), ROWS), :] = value * size[chunk, w]
            return carry

        lax.fori_loop(0, count, one_group, 0, unroll=2)

    def add_up(source, pitch, count, hot, store):
        def one_row(m, carry):
            value = source[pl.ds(m, count, stride=pitch), :]
            both = jnp.concatenate(split(value), axis=0)
            store(m, jnp.dot(hot, both, preferred_element_type=jnp.float32))
            return carry

        lax.fori_loop(0, ROWS, one_row, 0, unroll=8)

    def restore_one(chunk):
        half, first = chunk * ROWS // HALF, chunk * ROWS % HALF

        def one_source(w, carry):
            for pair in range(2):
                size = sizein_one[half, w, pair : pair + 1, :]
                for s in (w * 4 + pair * 2, w * 4 + pair * 2 + 1):
                    value = in_one[half, s, first : first + ROWS, :].astype(jnp.int32).astype(jnp.float32)
                    spread[pl.ds(pl.multiple_of(s * SPAN, 8), ROWS), :] = value * size
            return carry

        lax.fori_loop(0, 32, one_source, 0, unroll=2)

    def make_two(chunk):
        def keep(m, value):
            coarse_one[pl.ds(m, 64, stride=SPAN), :] = value

        if chunk * ROWS % HALF == 0:
            half = chunk * ROWS // HALF
            wait(sizein_one.at[half, pl.ds(0, 31)], sizeone_sem.at[1, half])
            wait(in_one.at[half, pl.ds(0, 124)], one_sem.at[1, half])
        restore_one(chunk)
        add_up(spread, SPAN, 128, hot_one, keep)
        quantize(coarse_one, 32, 2, chunk, out_two, size_two)
        here = pl.ds(v * 2, 2)
        in_two[chunk, here] = out_two[chunk, here]
        sizein_two[chunk, v] = size_two[chunk, v]

    def sends_two(chunk, step):
        w = dest_of(v, *step)
        send(
            size_two.at[chunk, w], sizein_two.at[chunk, v],
            sizetwo_sem.at[0, chunk], sizetwo_sem.at[1, chunk], (g, w),
        )
        send(
            out_two.at[chunk, pl.ds(w * 2, 2)], in_two.at[chunk, pl.ds(v * 2, 2)],
            two_sem.at[0, chunk], two_sem.at[1, chunk], (g, w),
        )

    def make_three(chunk):
        def keep(m, value):
            coarse_two[pl.ds(m, 32, stride=SPAN), :] = value

        wait(sizein_two.at[chunk, pl.ds(0, 31)], sizetwo_sem.at[1, chunk])
        wait(in_two.at[chunk, pl.ds(0, 62)], two_sem.at[1, chunk])
        restore(in_two, sizein_two, 32, 2, chunk)
        add_up(spread, SPAN, 64, hot_two, keep)
        quantize(coarse_two, 8, 4, chunk, out_three, size_three)
        here = pl.ds(g * 4, 4)
        in_three[chunk, here] = out_three[chunk, here]
        sizein_three[chunk, g] = size_three[chunk, g]

    def sends_three(chunk, step):
        h = lax.rem(g + step, 8)
        send(
            size_three.at[chunk, h], sizein_three.at[chunk, g],
            sizethree_sem.at[0, chunk], sizethree_sem.at[1, chunk], (h, v),
        )
        send(
            out_three.at[chunk, pl.ds(h * 4, 4)], in_three.at[chunk, pl.ds(g * 4, 4)],
            three_sem.at[0, chunk], three_sem.at[1, chunk], (h, v),
        )

    for chunk in range(EARLY):
        make_two(chunk)
        if chunk < AHEAD:
            for step in ORDER:
                sends_two(chunk, step)
    wait(zags_in.at[pl.ds(0, 7)], zags_sem.at[1])
    zags = jnp.sum(zags_in[...], axis=0)
    hot_three = one_hot(zags[0:1], 16)[:, :32]
    hot_three = jnp.concatenate([hot_three, hot_three], axis=1)
    relative[...] = weighted[...] * 32768.0 / jnp.sum(zags[1:2], axis=1, keepdims=True)
    for chunk in range(CHUNKS):
        ahead = chunk + AHEAD
        if chunk + EARLY < CHUNKS:
            make_two(chunk + EARLY)
        make_three(chunk)
        for place, step in enumerate(ORDER if ahead < CHUNKS else RING * 4):
            if place < len(RING):
                sends_three(chunk, RING[place])
            if ahead < CHUNKS:
                sends_two(ahead, step)

    for chunk in range(CHUNKS):
        wait(sizein_three.at[chunk, pl.ds(0, 7)], sizethree_sem.at[1, chunk])
        wait(in_three.at[chunk, pl.ds(0, 28)], three_sem.at[1, chunk])
        restore(in_three, sizein_three, 8, 4, chunk)

        def keep_three(m, value, chunk=chunk):
            graph[pl.ds(chunk * ROWS + m, 16, stride=BLOCK), :] = value

        add_up(spread, SPAN, 32, hot_three, keep_three)

    for half in range(2):
        wait(size_one.at[half, pl.ds(0, 31)], sizeone_sem.at[0, half])
        wait(out_one.at[half, pl.ds(0, 124)], one_sem.at[0, half])
    wait(tags_in.at[pl.ds(0, 31)], tags_sem.at[0])
    wait(zags_in.at[pl.ds(0, 7)], zags_sem.at[0])
    for chunk in range(CHUNKS):
        wait(size_two.at[chunk, pl.ds(0, 31)], sizetwo_sem.at[0, chunk])
        wait(out_two.at[chunk, pl.ds(0, 62)], two_sem.at[0, chunk])
        wait(size_three.at[chunk, pl.ds(0, 7)], sizethree_sem.at[0, chunk])
        wait(out_three.at[chunk, pl.ds(0, 28)], three_sem.at[0, chunk])


def per_device(
    blocks, ids_one, ids_two, ids_three, match_one, match_two, match_three,
    target_one, target_two, target_three, vertex_weights,
):
    del ids_two, ids_three
    vmem = pl.BlockSpec(memory_space=pltpu.VMEM)
    hbm = pl.BlockSpec(memory_space=pl.ANY)
    f32, i16, bf16 = jnp.float32, jnp.int16, jnp.bfloat16
    graph, relative = pl.pallas_call(
        kernel,
        out_shape=(
            jax.ShapeDtypeStruct((16 * BLOCK, BLOCK), f32),
            jax.ShapeDtypeStruct((1, BLOCK), f32),
        ),
        in_specs=[hbm, pl.BlockSpec(memory_space=pltpu.SMEM), hbm, hbm, hbm] + [vmem] * 4,
        out_specs=(vmem, vmem),
        scratch_shapes=[
            pltpu.VMEM((128, BLOCK, BLOCK), bf16),
            pltpu.VMEM((2, 128, HALF, BLOCK), i16),
            pltpu.VMEM((2, 128, HALF, BLOCK), i16),
            pltpu.VMEM((2, 32, 2, BLOCK), f32),
            pltpu.VMEM((2, 32, 2, BLOCK), f32),
            pltpu.VMEM((32, 2, BLOCK), f32),
            pltpu.VMEM((32, 2, BLOCK), f32),
            pltpu.VMEM((8, 2, BLOCK), f32),
            pltpu.VMEM((8, 2, BLOCK), f32),
            pltpu.VMEM((64 * SPAN, BLOCK), f32),
            pltpu.VMEM((CHUNKS, 64, ROWS, BLOCK), i16),
            pltpu.VMEM((CHUNKS, 64, ROWS, BLOCK), i16),
            pltpu.VMEM((CHUNKS, 32, 1, BLOCK), f32),
            pltpu.VMEM((CHUNKS, 32, 1, BLOCK), f32),
            pltpu.VMEM((128 * SPAN, BLOCK), f32),
            pltpu.VMEM((32 * SPAN, BLOCK), f32),
            pltpu.VMEM((CHUNKS, 32, ROWS, BLOCK), i16),
            pltpu.VMEM((CHUNKS, 32, ROWS, BLOCK), i16),
            pltpu.VMEM((CHUNKS, 8, 1, BLOCK), f32),
            pltpu.VMEM((CHUNKS, 8, 1, BLOCK), f32),
            pltpu.VMEM((1, BLOCK), f32),
            pltpu.VMEM(match_one.shape, jnp.int32),
            pltpu.VMEM(match_two.shape, jnp.int32),
            pltpu.VMEM(match_three.shape, jnp.int32),
            pltpu.VMEM((8, BLOCK), f32),
            pltpu.VMEM((4 * BLOCK, BLOCK), f32),
            pltpu.SemaphoreType.DMA((3,)),
            pltpu.SemaphoreType.DMA((32,)),
            pltpu.SemaphoreType.DMA((2, 2)),
            pltpu.SemaphoreType.DMA((2, 2)),
            pltpu.SemaphoreType.DMA((2,)),
            pltpu.SemaphoreType.DMA((2,)),
            pltpu.SemaphoreType.DMA((2, CHUNKS)),
            pltpu.SemaphoreType.DMA((2, CHUNKS)),
            pltpu.SemaphoreType.DMA((2, CHUNKS)),
            pltpu.SemaphoreType.DMA((2, CHUNKS)),
        ],
        compiler_params=pltpu.CompilerParams(
            collective_id=0, has_side_effects=True, vmem_limit_bytes=56 * 2**20
        ),
        name="coarsen",
    )(
        blocks, ids_one, match_one, match_two, match_three,
        target_one.reshape(1, -1), target_two.reshape(1, -1), target_three.reshape(1, -1), vertex_weights,
    )
    return graph.reshape(16, BLOCK, BLOCK), relative


def solution(mesh):
    both = ("grp", "dev")
    in_specs = (
        P(both, None, None), P(None, both), P(None, both), P(None, both), P(), P(), P(),
        P(both), P(both), P(both), P(both, None),
    )
    return jax.shard_map(
        per_device, mesh=mesh, in_specs=in_specs, out_specs=(P(both, None, None), P(both, None)), check_vma=False
    )
```

```python
import functools

import jax
import jax.numpy as jnp
from jax import lax
from jax.experimental import pallas as pl
from jax.experimental.pallas import tpu as pltpu
from jax.sharding import PartitionSpec as P

MESH = pl.DeviceIdType.MESH
BLOCK = 128
CHUNKS = 8
EARLY = 4
AHEAD = 3
HALF = BLOCK // 2
ROWS = BLOCK // CHUNKS
SPAN = ROWS + 8
TOP = 32767.0
TINY = 1e-30
PARTS = 4
ROUNDS = (
    ((2, 2),),
    ((0, 1), (1, 1), (0, 3), (3, 3)),
    ((1, 0), (1, 3), (3, 0), (3, 1)),
    ((0, 2), (2, 1), (2, 3)),
    ((2, 0), (1, 2), (3, 2)),
    ((0, 0),),
)
ORDER = tuple(
    (dx, dy, dc) for turn in ROUNDS for dc in (0, 1) for dx, dy in turn if (dx, dy, dc) != (0, 0, 0)
)
RING = (1, 7, 2, 6, 3, 5, 4)


def dest_of(v, dx, dy, dc):
    x, y, c = v // 8, lax.rem(v // 2, 4), lax.rem(v, 2)
    ddx = jnp.where(c == 1, dy, dx)
    ddy = jnp.where(c == 1, dx, dy)
    return lax.rem(x + ddx, 4) * 8 + lax.rem(y + ddy, 4) * 2 + lax.rem(c + dc, 2)


def dest_at(v, turn):
    code = jnp.int32(0)
    for place, (dx, dy, dc) in enumerate(ORDER):
        code = jnp.where(turn == place, dx * 8 + dy * 2 + dc, code)
    return dest_of(v, code // 8, lax.rem(code // 2, 4), lax.rem(code, 2))


def split(value):
    high = value.astype(jnp.bfloat16)
    return high, (value - high.astype(jnp.float32)).astype(jnp.bfloat16)


def one_hot(lanes, count):
    width = lanes.shape[1]
    rows = lax.broadcasted_iota(jnp.int32, (count, width), 0).astype(jnp.float32)
    return jnp.where(rows == lanes, 1.0, 0.0).astype(jnp.bfloat16)


def send(src, dst, send_sem, recv_sem, device):
    pltpu.make_async_remote_copy(
        src_ref=src, dst_ref=dst, send_sem=send_sem, recv_sem=recv_sem, device_id=device, device_id_type=MESH
    ).start()


def wait(ref, sem):
    pltpu.make_async_copy(ref, ref, sem).wait()


def kernel(
    blocks, ids, one_hbm, two_hbm, three_hbm, target_one, target_two, target_three, weights,
    graph, relative,
    fine, out_one, in_one, size_one, sizein_one, tags_out, tags_in, zags_out, zags_in, coarse_one, out_two, in_two,
    size_two, sizein_two, spread, coarse_two, out_three, in_three, size_three, sizein_three, weighted,
    one, two, three, maps, projected, tables_sem, fine_sem, one_sem, sizeone_sem, tags_sem, zags_sem,
    two_sem, sizetwo_sem, three_sem, sizethree_sem,
):
    g, v = lax.axis_index("grp"), lax.axis_index("dev")
    barrier = pltpu.get_barrier_semaphore()
    for step in ORDER:
        pl.semaphore_signal(barrier, inc=1, device_id=(g, dest_of(v, *step)), device_id_type=MESH)
    for step in RING:
        pl.semaphore_signal(barrier, inc=1, device_id=(lax.rem(g + step, 8), v), device_id_type=MESH)
    tables = [
        pltpu.make_async_copy(source, table, tables_sem.at[place])
        for place, (source, table) in enumerate(((one_hbm, one), (two_hbm, two), (three_hbm, three)))
    ]
    for table in tables:
        table.start()
    for place, step in enumerate(ORDER + ((0, 0, 0),)):
        some = pl.ds(dest_of(v, *step) * 4, 4)
        pltpu.make_async_copy(blocks.at[some], fine.at[some], fine_sem.at[place]).start()

    def composed(numbers):
        first = jnp.concatenate([one[pl.ds(n, 1), :] for n in numbers], axis=0)
        second = jnp.concatenate([two[pl.ds(n // 2, 1), :] for n in numbers], axis=0)
        third = jnp.concatenate([three[pl.ds(n // 4, 1), :] for n in numbers], axis=0)
        second = jnp.take_along_axis(second, first, axis=1)
        return jnp.take_along_axis(third, second, axis=1).astype(jnp.float32)

    for table in tables:
        table.wait()

    def find_maps(turn):
        w = dest_at(v, turn)
        maps[...] = composed([ids[a, w * 4 + j] for a in range(2) for j in range(4)])

    def project(turn):
        w = dest_at(v, turn)
        wait(fine.at[pl.ds(w * 4, 4)], fine_sem.at[turn])
        here = maps[...]
        for j in range(4):
            left = one_hot(here[j : j + 1], BLOCK)
            right = one_hot(here[4 + j : 5 + j], BLOCK)
            halfway = jnp.dot(left, fine[w * 4 + j], preferred_element_type=jnp.float32)
            both = jnp.concatenate(split(halfway), axis=0)
            full = lax.dot_general(both, right, (((1,), (1,)), ((), ())), preferred_element_type=jnp.float32)
            projected[j * BLOCK : (j + 1) * BLOCK, :] = full[:BLOCK] + full[BLOCK:]

    def round_one(turn):
        w = dest_at(v, turn)
        for pair in range(2):
            for half in range(2):
                starts = [(pair * 2 + k) * BLOCK + half * HALF for k in range(2)]
                values = [projected[start : start + HALF, :] for start in starts]
                top = jnp.maximum(*[jnp.max(jnp.abs(a), axis=0, keepdims=True) for a in values])
                top = jnp.maximum(top, TINY)
                factor = TOP / top
                for k, a in enumerate(values):
                    out_one[half, w * 4 + pair * 2 + k] = jnp.round(a * factor).astype(jnp.int32).astype(jnp.int16)
                size_one[half, w, pair : pair + 1, :] = top * (1.0 / TOP)

    def send_one(half, turn):
        w = dest_at(v, turn)
        send(
            size_one.at[half, w], sizein_one.at[half, v], sizeone_sem.at[0, half], sizeone_sem.at[1, half], (g, w)
        )
        send(
            out_one.at[half, pl.ds(w * 4, 4)], in_one.at[half, pl.ds(v * 4, 4)],
            one_sem.at[0, half], one_sem.at[1, half], (g, w),
        )

    find_maps(0)
    project(0)
    find_maps(1)
    pl.semaphore_wait(barrier, len(ORDER) + len(RING))
    def step_on(turn, carry):
        round_one(turn - 1)
        project(turn)
        find_maps(jnp.minimum(turn + 1, 31))
        send_one(0, turn - 1)
        return carry

    lax.fori_loop(1, 32, step_on, 0)
    round_one(31)

    lane = lax.broadcasted_iota(jnp.int32, (32, BLOCK), 1)
    row = lax.broadcasted_iota(jnp.int32, (32, BLOCK), 0)
    local = weights[...]
    partial = jnp.sum(jnp.sum(local, axis=0, keepdims=True), axis=1, keepdims=True)

    def spread_tags(table, per, rows, lanes, place):
        table = jnp.concatenate([table] * (BLOCK // table.shape[1]), axis=1)
        table = jnp.broadcast_to(table, lanes.shape)
        picked = jnp.take_along_axis(table, rows * per + lax.rem(lanes, per), axis=1)
        return jnp.where(lanes // per == place, picked, 0).astype(jnp.float32)

    tags_one = spread_tags(target_one[...], 4, row, lane, v)
    tags_two = spread_tags(target_two[...], 2, row, lane, v)
    tags_two = tags_two + jnp.where(lane == v + 64, partial, 0.0)
    for w in range(32):
        tags_out[w, 0:1, :] = tags_one[w : w + 1]
        tags_out[w, 1:2, :] = tags_two[w : w + 1]
    tags_in[v] = tags_out[v]

    for step in ORDER:
        w = dest_of(v, *step)
        send(tags_out.at[w], tags_in.at[v], tags_sem.at[0], tags_sem.at[1], (g, w))
    lax.fori_loop(0, 31, lambda turn, carry: (send_one(1, turn), carry)[1], 0)
    for half in range(2):
        in_one[half, pl.ds(v * 4, 4)] = out_one[half, pl.ds(v * 4, 4)]
        sizein_one[half, v] = size_one[half, v]

    base = (g * 32 + v) * 8
    own = composed([base + e for e in range(8)])
    part = lax.broadcasted_iota(jnp.int32, (8, BLOCK), 0)
    total_here = jnp.zeros((8, BLOCK), jnp.float32)
    up = lax.broadcasted_iota(jnp.int32, (BLOCK, BLOCK), 0).astype(jnp.float32)
    for e in range(8):
        hot = jnp.where(up == own[e : e + 1], 1.0, 0.0)
        total_here = total_here + lax.dot_general(
            jnp.where(part == e, local, 0.0), hot, (((1,), (1,)), ((), ())),
            precision=lax.Precision.HIGHEST, preferred_element_type=jnp.float32,
        )
    weighted[...] = jnp.sum(total_here, axis=0, keepdims=True)

    wait(tags_in.at[pl.ds(0, 31)], tags_sem.at[1])
    tags = jnp.sum(tags_in[...], axis=0)
    hot_one = one_hot(tags[0:1], 64)
    hot_one = jnp.concatenate([hot_one, hot_one], axis=1)
    hot_two = one_hot(tags[1:2], 32)[:, :64]
    hot_two = jnp.concatenate([hot_two, hot_two], axis=1)
    beyond = lax.broadcasted_iota(jnp.int32, (1, BLOCK), 1)
    group_total = jnp.sum(jnp.where(beyond >= 64, tags[1:2], 0.0), axis=1, keepdims=True)

    lane8 = lax.broadcasted_iota(jnp.int32, (8, BLOCK), 1)
    row8 = lax.broadcasted_iota(jnp.int32, (8, BLOCK), 0)
    tags_three = spread_tags(target_three[...], 4, row8, lane8, g)
    totals = jnp.where(beyond == g, group_total, 0.0)
    for h in range(8):
        zags_out[h, 0:1, :] = tags_three[h : h + 1]
        zags_out[h, 1:2, :] = totals
    zags_in[g] = zags_out[g]
    for step in RING:
        h = lax.rem(g + step, 8)
        send(zags_out.at[h], zags_in.at[g], zags_sem.at[0], zags_sem.at[1], (h, v))

    def quantize(source, count, per, chunk, out, size):
        def one_group(w, carry):
            values = [
                source[pl.ds(pl.multiple_of((w * per + k) * SPAN, 8), ROWS), :] for k in range(per)
            ]
            top = functools.reduce(jnp.maximum, [jnp.max(jnp.abs(a), axis=0, keepdims=True) for a in values])
            top = jnp.maximum(top, TINY)
            factor = TOP / top
            for k, a in enumerate(values):
                out[chunk, w * per + k] = jnp.round(a * factor).astype(jnp.int32).astype(jnp.int16)
            size[chunk, w] = top * (1.0 / TOP)
            return carry

        lax.fori_loop(0, count, one_group, 0, unroll=2)

    def restore(source, size, count, per, chunk):
        def one_group(w, carry):
            for k in range(per):
                s = w * per + k
                value = source[chunk, s].astype(jnp.int32).astype(jnp.float32)
                spread[pl.ds(pl.multiple_of(s * SPAN, 8), ROWS), :] = value * size[chunk, w]
            return carry

        lax.fori_loop(0, count, one_group, 0, unroll=2)

    def add_up(source, pitch, count, hot, store):
        def one_row(m, carry):
            value = source[pl.ds(m, count, stride=pitch), :]
            both = jnp.concatenate(split(value), axis=0)
            store(m, jnp.dot(hot, both, preferred_element_type=jnp.float32))
            return carry

        lax.fori_loop(0, ROWS, one_row, 0, unroll=8)

    def restore_one(chunk):
        half, first = chunk * ROWS // HALF, chunk * ROWS % HALF

        def one_source(w, carry):
            for pair in range(2):
                size = sizein_one[half, w, pair : pair + 1, :]
                for s in (w * 4 + pair * 2, w * 4 + pair * 2 + 1):
                    value = in_one[half, s, first : first + ROWS, :].astype(jnp.int32).astype(jnp.float32)
                    spread[pl.ds(pl.multiple_of(s * SPAN, 8), ROWS), :] = value * size
            return carry

        lax.fori_loop(0, 32, one_source, 0, unroll=2)

    def make_two(chunk):
        def keep(m, value):
            coarse_one[pl.ds(m, 64, stride=SPAN), :] = value

        if chunk * ROWS % HALF == 0:
            half = chunk * ROWS // HALF
            wait(sizein_one.at[half, pl.ds(0, 31)], sizeone_sem.at[1, half])
            wait(in_one.at[half, pl.ds(0, 124)], one_sem.at[1, half])
        restore_one(chunk)
        add_up(spread, SPAN, 128, hot_one, keep)
        quantize(coarse_one, 32, 2, chunk, out_two, size_two)
        here = pl.ds(v * 2, 2)
        in_two[chunk, here] = out_two[chunk, here]
        sizein_two[chunk, v] = size_two[chunk, v]

    def sends_two(chunk, step):
        w = dest_of(v, *step)
        send(
            size_two.at[chunk, w], sizein_two.at[chunk, v],
            sizetwo_sem.at[0, chunk], sizetwo_sem.at[1, chunk], (g, w),
        )
        send(
            out_two.at[chunk, pl.ds(w * 2, 2)], in_two.at[chunk, pl.ds(v * 2, 2)],
            two_sem.at[0, chunk], two_sem.at[1, chunk], (g, w),
        )

    def make_three(chunk):
        def keep(m, value):
            coarse_two[pl.ds(m, 32, stride=SPAN), :] = value

        wait(sizein_two.at[chunk, pl.ds(0, 31)], sizetwo_sem.at[1, chunk])
        wait(in_two.at[chunk, pl.ds(0, 62)], two_sem.at[1, chunk])
        restore(in_two, sizein_two, 32, 2, chunk)
        add_up(spread, SPAN, 64, hot_two, keep)
        quantize(coarse_two, 8, 4, chunk, out_three, size_three)
        here = pl.ds(g * 4, 4)
        in_three[chunk, here] = out_three[chunk, here]
        sizein_three[chunk, g] = size_three[chunk, g]

    def sends_three(chunk, step):
        h = lax.rem(g + step, 8)
        send(
            size_three.at[chunk, h], sizein_three.at[chunk, g],
            sizethree_sem.at[0, chunk], sizethree_sem.at[1, chunk], (h, v),
        )
        send(
            out_three.at[chunk, pl.ds(h * 4, 4)], in_three.at[chunk, pl.ds(g * 4, 4)],
            three_sem.at[0, chunk], three_sem.at[1, chunk], (h, v),
        )

    for chunk in range(EARLY):
        make_two(chunk)
        if chunk < AHEAD:
            for step in ORDER:
                sends_two(chunk, step)
    wait(zags_in.at[pl.ds(0, 7)], zags_sem.at[1])
    zags = jnp.sum(zags_in[...], axis=0)
    hot_three = one_hot(zags[0:1], 16)[:, :32]
    hot_three = jnp.concatenate([hot_three, hot_three], axis=1)
    relative[...] = weighted[...] * 32768.0 / jnp.sum(zags[1:2], axis=1, keepdims=True)
    for chunk in range(CHUNKS):
        ahead = chunk + AHEAD
        if chunk + EARLY < CHUNKS:
            make_two(chunk + EARLY)
        make_three(chunk)
        for place, step in enumerate(ORDER if ahead < CHUNKS else RING * 4):
            if place < len(RING):
                sends_three(chunk, RING[place])
            if ahead < CHUNKS:
                sends_two(ahead, step)

    for chunk in range(CHUNKS):
        wait(sizein_three.at[chunk, pl.ds(0, 7)], sizethree_sem.at[1, chunk])
        wait(in_three.at[chunk, pl.ds(0, 28)], three_sem.at[1, chunk])
        restore(in_three, sizein_three, 8, 4, chunk)

        def keep_three(m, value, chunk=chunk):
            graph[pl.ds(chunk * ROWS + m, 16, stride=BLOCK), :] = value

        add_up(spread, SPAN, 32, hot_three, keep_three)

    for half in range(2):
        wait(size_one.at[half, pl.ds(0, 31)], sizeone_sem.at[0, half])
        wait(out_one.at[half, pl.ds(0, 124)], one_sem.at[0, half])
    wait(tags_in.at[pl.ds(0, 31)], tags_sem.at[0])
    wait(zags_in.at[pl.ds(0, 7)], zags_sem.at[0])
    for chunk in range(CHUNKS):
        wait(size_two.at[chunk, pl.ds(0, 31)], sizetwo_sem.at[0, chunk])
        wait(out_two.at[chunk, pl.ds(0, 62)], two_sem.at[0, chunk])
        wait(size_three.at[chunk, pl.ds(0, 7)], sizethree_sem.at[0, chunk])
        wait(out_three.at[chunk, pl.ds(0, 28)], three_sem.at[0, chunk])


def copy_kernel(graph, relative, graph_out, relative_out, held, in_sem, out_sem):
    part = graph.shape[0] // PARTS
    ins, outs = [], []
    for place in range(PARTS):
        here = pl.ds(place * part, part)
        ins.append(pltpu.make_async_copy(graph.at[here], held.at[here], in_sem.at[place]))
        outs.append(pltpu.make_async_copy(held.at[here], graph_out.at[here], out_sem.at[place]))
    for copy in ins:
        copy.start()
    relative_out[...] = relative[...]
    for before, after in zip(ins, outs):
        before.wait()
        after.start()
    for copy in outs:
        copy.wait()


def per_device(
    blocks, ids_one, ids_two, ids_three, match_one, match_two, match_three,
    target_one, target_two, target_three, vertex_weights,
):
    del ids_two, ids_three
    vmem = pl.BlockSpec(memory_space=pltpu.VMEM)
    hbm = pl.BlockSpec(memory_space=pl.ANY)
    f32, i16, bf16 = jnp.float32, jnp.int16, jnp.bfloat16
    graph, relative = pl.pallas_call(
        kernel,
        out_shape=(
            jax.ShapeDtypeStruct((16 * BLOCK, BLOCK), f32),
            jax.ShapeDtypeStruct((1, BLOCK), f32),
        ),
        in_specs=[hbm, pl.BlockSpec(memory_space=pltpu.SMEM), hbm, hbm, hbm] + [vmem] * 4,
        out_specs=(vmem, vmem),
        scratch_shapes=[
            pltpu.VMEM((128, BLOCK, BLOCK), bf16),
            pltpu.VMEM((2, 128, HALF, BLOCK), i16),
            pltpu.VMEM((2, 128, HALF, BLOCK), i16),
            pltpu.VMEM((2, 32, 2, BLOCK), f32),
            pltpu.VMEM((2, 32, 2, BLOCK), f32),
            pltpu.VMEM((32, 2, BLOCK), f32),
            pltpu.VMEM((32, 2, BLOCK), f32),
            pltpu.VMEM((8, 2, BLOCK), f32),
            pltpu.VMEM((8, 2, BLOCK), f32),
            pltpu.VMEM((64 * SPAN, BLOCK), f32),
            pltpu.VMEM((CHUNKS, 64, ROWS, BLOCK), i16),
            pltpu.VMEM((CHUNKS, 64, ROWS, BLOCK), i16),
            pltpu.VMEM((CHUNKS, 32, 1, BLOCK), f32),
            pltpu.VMEM((CHUNKS, 32, 1, BLOCK), f32),
            pltpu.VMEM((128 * SPAN, BLOCK), f32),
            pltpu.VMEM((32 * SPAN, BLOCK), f32),
            pltpu.VMEM((CHUNKS, 32, ROWS, BLOCK), i16),
            pltpu.VMEM((CHUNKS, 32, ROWS, BLOCK), i16),
            pltpu.VMEM((CHUNKS, 8, 1, BLOCK), f32),
            pltpu.VMEM((CHUNKS, 8, 1, BLOCK), f32),
            pltpu.VMEM((1, BLOCK), f32),
            pltpu.VMEM(match_one.shape, jnp.int32),
            pltpu.VMEM(match_two.shape, jnp.int32),
            pltpu.VMEM(match_three.shape, jnp.int32),
            pltpu.VMEM((8, BLOCK), f32),
            pltpu.VMEM((4 * BLOCK, BLOCK), f32),
            pltpu.SemaphoreType.DMA((3,)),
            pltpu.SemaphoreType.DMA((32,)),
            pltpu.SemaphoreType.DMA((2, 2)),
            pltpu.SemaphoreType.DMA((2, 2)),
            pltpu.SemaphoreType.DMA((2,)),
            pltpu.SemaphoreType.DMA((2,)),
            pltpu.SemaphoreType.DMA((2, CHUNKS)),
            pltpu.SemaphoreType.DMA((2, CHUNKS)),
            pltpu.SemaphoreType.DMA((2, CHUNKS)),
            pltpu.SemaphoreType.DMA((2, CHUNKS)),
        ],
        compiler_params=pltpu.CompilerParams(
            collective_id=0, has_side_effects=True, vmem_limit_bytes=56 * 2**20
        ),
        name="coarsen",
    )(
        blocks, ids_one, match_one, match_two, match_three,
        target_one.reshape(1, -1), target_two.reshape(1, -1), target_three.reshape(1, -1), vertex_weights,
    )
    graph, relative = pl.pallas_call(
        copy_kernel,
        out_shape=(jax.ShapeDtypeStruct(graph.shape, f32), jax.ShapeDtypeStruct(relative.shape, f32)),
        in_specs=[hbm, vmem],
        out_specs=(hbm, vmem),
        scratch_shapes=[
            pltpu.VMEM(graph.shape, f32),
            pltpu.SemaphoreType.DMA((PARTS,)),
            pltpu.SemaphoreType.DMA((PARTS,)),
        ],
        name="put_out",
    )(graph, relative)
    return graph.reshape(16, BLOCK, BLOCK), relative


def solution(mesh):
    both = ("grp", "dev")
    in_specs = (
        P(both, None, None), P(None, both), P(None, both), P(None, both), P(), P(), P(),
        P(both), P(both), P(both), P(both, None),
    )
    return jax.shard_map(
        per_device, mesh=mesh, in_specs=in_specs, out_specs=(P(both, None, None), P(both, None)), check_vma=False
    )
```
